16 devices in a mesh: data: 16 (over z, y, x, core).
Axes of the slice: x: 2, y: 2, z: 2, core: 2. Of those that a mesh axis runs over, the one named last changes fastest.
Arguments:
- x_now: bfloat16 [128, 196, 768], P('data')
- x_next: bfloat16 [128, 196, 768], P('data')
- labels: int32 [128], P('data')
- w_up: float32 [8, 768, 3072], replicated
- w_down: float32 [8, 3072, 768], replicated
- w_head: float32 [768, 1000], replicated
- mom_up: float32 [8, 768, 3072], P(None, None, 'data')
- mom_down: float32 [8, 3072, 768], P(None, 'data')
- mom_head: float32 [768, 1000], P('data')
- learn_rate: float32 [], replicated
- mom_decay: float32 [], replicated
Outputs:
- output 1: float32 [128, 1000], P('data')
- output 2: float32 [8, 768, 3072], replicated
- output 3: float32 [8, 3072, 768], replicated
- output 4: float32 [768, 1000], replicated
- output 5: float32 [8, 768, 3072], P(None, None, 'data')
- output 6: float32 [8, 3072, 768], P(None, 'data')
- output 7: float32 [768, 1000], P('data')
All inputs are finite; a program needn't handle non-finite values.
Results may differ from the reference program's by a relative error of at most 0.0121511.
Values are sent between devices in bfloat16 or wider.
A program may use at most 1.25 GiB of HBM per device.

```python
import math
import jax
import jax.numpy as jnp
from jax import lax

BATCH_DEV = 8
TOKENS = 196
WIDTH = 768
HIDDEN = 3072
CLASSES = 1000
LAYERS = 8
GROUPS = 16
LN_EPS = 1e-6


def setup_inputs(seed: int = 0) -> dict:
    keys = jax.random.split(jax.random.key(seed), 13)
    batch = GROUPS * BATCH_DEV
    mom_scale = batch ** -0.5
    img_now = jax.random.normal(keys[0], (batch, 1, WIDTH), jnp.float32)
    tok_now = jax.random.normal(keys[1], (batch, TOKENS, WIDTH), jnp.float32)
    img_next = jax.random.normal(keys[2], (batch, 1, WIDTH), jnp.float32)
    tok_next = jax.random.normal(keys[3], (batch, TOKENS, WIDTH), jnp.float32)
    down_raw = jax.random.normal(keys[6], (LAYERS, HIDDEN, WIDTH), jnp.float32) * HIDDEN ** -0.5
    mom_raw = jax.random.normal(keys[9], (LAYERS, HIDDEN, WIDTH), jnp.float32) * (HIDDEN ** -0.5 * mom_scale)
    return {
        "x_now": (0.8 * img_now + 0.6 * tok_now).astype(jnp.bfloat16),
        "x_next": (0.8 * img_next + 0.6 * tok_next).astype(jnp.bfloat16),
        "labels": jax.random.randint(keys[4], (batch,), 0, CLASSES, jnp.int32),
        "w_up": jax.random.normal(keys[5], (LAYERS, WIDTH, HIDDEN), jnp.float32) * WIDTH ** -0.5,
        "w_down": down_raw - jnp.mean(down_raw, axis=1, keepdims=True),
        "w_head": jax.random.normal(keys[7], (WIDTH, CLASSES), jnp.float32) * WIDTH ** -0.5,
        "mom_up": jax.random.normal(keys[8], (LAYERS, WIDTH, HIDDEN), jnp.float32) * (WIDTH ** -0.5 * mom_scale),
        "mom_down": mom_raw - jnp.mean(mom_raw, axis=1, keepdims=True),
        "mom_head": jax.random.normal(keys[10], (WIDTH, CLASSES), jnp.float32) * (WIDTH ** -0.5 * mom_scale),
        "learn_rate": jax.random.uniform(keys[11], (), jnp.float32, 0.3, 0.6) * math.sqrt(batch),
        "mom_decay": jax.random.uniform(keys[12], (), jnp.float32, 0.7, 0.95),
    }


def norm_rows(values):
    mean_v = jnp.mean(values, axis=-1, keepdims=True)
    centered = values - mean_v
    var_v = jnp.mean(centered * centered, axis=-1, keepdims=True)
    return centered * lax.rsqrt(var_v + LN_EPS)


def block_fwd(x_rows, w_in, w_out):
    x_wide = x_rows.astype(jnp.float32)
    u_rows = norm_rows(x_wide).astype(jnp.bfloat16)
    pre_act = jnp.dot(u_rows, w_in.astype(jnp.bfloat16), preferred_element_type=jnp.float32).astype(jnp.bfloat16)
    gelu_out = jax.nn.gelu(pre_act.astype(jnp.float32), approximate=True).astype(jnp.bfloat16)
    block_out = jnp.dot(gelu_out, w_out.astype(jnp.bfloat16), preferred_element_type=jnp.float32).astype(jnp.bfloat16)
    return (x_wide + block_out.astype(jnp.float32)).astype(jnp.bfloat16)


def group_logits(x_grp, w_up, w_down, w_head):
    n_img, n_tok, width = x_grp.shape

    def layer_step(rows, layer_w):
        return block_fwd(rows, layer_w[0], layer_w[1]), None

    rows, _ = lax.scan(layer_step, x_grp.reshape(n_img * n_tok, width), (w_up, w_down))
    pooled = jnp.mean(rows.reshape(n_img, n_tok, width), axis=1, dtype=jnp.float32)
    normed = norm_rows(pooled).astype(jnp.bfloat16)
    return jnp.dot(normed, w_head.astype(jnp.bfloat16), preferred_element_type=jnp.float32)


def cross_ent(logits, labels):
    log_norm = jax.nn.logsumexp(logits, axis=-1)
    picked = jnp.sum(logits * jax.nn.one_hot(labels, logits.shape[-1], dtype=logits.dtype), axis=-1)
    return log_norm - picked


def reference(x_now, x_next, labels, w_up, w_down, w_head, mom_up, mom_down, mom_head, learn_rate, mom_decay):
    weights = (w_up, w_down, w_head)
    batch_total = GROUPS * BATCH_DEV
    x_groups = x_now.reshape(GROUPS, BATCH_DEV, TOKENS, WIDTH)
    label_groups = labels.reshape(GROUPS, BATCH_DEV)

    def accumulate(total, group):
        x_grp, lab_grp = group

        def group_loss(params):
            logits = group_logits(x_grp, params[0], params[1], params[2])
            return jnp.sum(cross_ent(logits, lab_grp)) / batch_total

        _, loss_pull = jax.vjp(group_loss, weights)
        gradients = loss_pull(jnp.ones((), jnp.float32))[0]
        return (total[0] + gradients[0], total[1] + gradients[1], total[2] + gradients[2]), None

    zero_grads = (jnp.zeros_like(w_up), jnp.zeros_like(w_down), jnp.zeros_like(w_head))
    gradients, _ = lax.scan(accumulate, zero_grads, (x_groups, label_groups))
    new_mom_up = mom_decay * mom_up + gradients[0]
    new_mom_down = mom_decay * mom_down + gradients[1]
    new_mom_head = mom_decay * mom_head + gradients[2]
    new_w_up = w_up - learn_rate * new_mom_up
    new_w_down = w_down - learn_rate * new_mom_down
    new_w_head = w_head - learn_rate * new_mom_head
    next_groups = x_next.reshape(GROUPS, BATCH_DEV, TOKENS, WIDTH)
    logits_next = lax.map(lambda x_grp: group_logits(x_grp, new_w_up, new_w_down, new_w_head), next_groups)
    logits_next = logits_next.reshape(GROUPS * BATCH_DEV, CLASSES)
    return (logits_next, new_w_up, new_w_down, new_w_head, new_mom_up, new_mom_down, new_mom_head)
```

```python
import functools

import jax
import jax.numpy as jnp
from jax import lax
from jax.experimental import pallas as pl
from jax.experimental.pallas import tpu as pltpu
from jax.sharding import PartitionSpec as P

LN_EPS = 1e-6
CONTRACT_ROWS = (((0,), (0,)), ((), ()))
CONTRACT_LAST = (((1,), (1,)), ((), ()))
TANH_A = 0.7978845608028654
TANH_B = 0.7978845608028654 * 0.044715
VMEM_BYTES = 67000000


def norm_rows(values):
    mean_v = jnp.mean(values, axis=-1, keepdims=True)
    centered = values - mean_v
    var_v = jnp.mean(centered * centered, axis=-1, keepdims=True)
    return centered * lax.rsqrt(var_v + LN_EPS)


def norm_rows_back(values, cot):
    mean_v = jnp.mean(values, axis=-1, keepdims=True)
    centered = values - mean_v
    var_v = jnp.mean(centered * centered, axis=-1, keepdims=True)
    rstd = lax.rsqrt(var_v + LN_EPS)
    hat = centered * rstd
    mean_c = jnp.mean(cot, axis=-1, keepdims=True)
    mean_h = jnp.mean(cot * hat, axis=-1, keepdims=True)
    return rstd * (cot - mean_c - hat * mean_h)


def gelu_parts(values):
    squared = values * values
    tanh_v = jnp.tanh(values * (TANH_A + TANH_B * squared))
    cdf = 0.5 + 0.5 * tanh_v
    return values * cdf, cdf, tanh_v, squared


def row_chunk(n_rows):
    for size in (224, 256, 128, 64, 32, 16):
        if n_rows % size == 0:
            return size
    return n_rows


def tile_of(hidden):
    for size in (768, 384):
        if hidden % size == 0:
            return size
    return hidden


def forward_kernel(save, update, rows_step, *refs):
    refs = list(refs)
    x_ref, up_ref, down_ref = refs[:3]
    refs = refs[3:]
    if update:
        step_up_ref, step_down_ref = refs[:2]
        refs = refs[2:]
        refs = refs[update - 1:]
        new_up_ref, new_down_ref = refs[:2]
        refs = refs[2:]
    if save:
        act_ref, saved_ref = refs[:2]
        refs = refs[2:]
    out_ref, rows_ref, normed_ref, total_ref = refs
    layer, tile = pl.program_id(0), pl.program_id(1)
    n_rows = x_ref.shape[0]

    @pl.when((layer == 0) & (tile == 0))
    def _():
        rows_ref[...] = x_ref[...]

    @pl.when(tile == 0)
    def _():
        for start in range(0, n_rows, rows_step):
            part = rows_ref[start:start + rows_step, :]
            normed_ref[start:start + rows_step, :] = norm_rows(part.astype(jnp.float32)).astype(jnp.bfloat16)
            if save:
                saved_ref[start:start + rows_step, :] = part
        total_ref[...] = jnp.zeros_like(total_ref)

    up_w = up_ref[...]
    down_w = down_ref[...]
    if update:
        up_w = up_w - step_up_ref[...].astype(jnp.float32).T
        down_w = down_w - step_down_ref[...].astype(jnp.float32)
        new_up_ref[...] = up_w
        new_down_ref[...] = down_w
    up_w = up_w.astype(jnp.bfloat16)
    down_w = down_w.astype(jnp.bfloat16)
    for start in range(0, n_rows, rows_step):
        here = slice(start, start + rows_step)
        pre = jnp.dot(normed_ref[here, :], up_w, preferred_element_type=jnp.float32).astype(jnp.bfloat16)
        if save:
            act_ref[here, :] = pre
        gelu_v = gelu_parts(pre.astype(jnp.float32))[0].astype(jnp.bfloat16)
        total_ref[here, :] += jnp.dot(gelu_v, down_w, preferred_element_type=jnp.float32)

    @pl.when(tile == pl.num_programs(1) - 1)
    def _():
        for start in range(0, n_rows, rows_step):
            here = slice(start, start + rows_step)
            block = total_ref[here, :].astype(jnp.bfloat16).astype(jnp.float32)
            rows_ref[here, :] = (rows_ref[here, :].astype(jnp.float32) + block).astype(jnp.bfloat16)

    @pl.when((tile == pl.num_programs(1) - 1) & (layer == pl.num_programs(0) - 1))
    def _():
        out_ref[...] = rows_ref[...]


def forward_stack(x_rows, w_up, w_down, layers, save, steps=None, held=None):
    n_rows, width = x_rows.shape
    hidden = w_up.shape[2]
    tile = tile_of(hidden)
    first, n_layers = layers[0], len(layers)
    whole = pl.BlockSpec((n_rows, width), lambda l, h: (0, 0))
    up_spec = pl.BlockSpec((None, width, tile), lambda l, h: (first + l, 0, h))
    down_spec = pl.BlockSpec((None, tile, width), lambda l, h: (first + l, h, 0))
    in_specs = [whole, up_spec, down_spec]
    args = [x_rows, w_up, w_down]
    out_shape, out_specs, aliases = [], [], {}
    update = 0
    if steps is not None:
        update = 1
        last = 2 * (n_layers - 1)
        in_specs.append(pl.BlockSpec((None, tile, width), lambda l, h: (last - 2 * l, h, 0)))
        in_specs.append(pl.BlockSpec((None, tile, width), lambda l, h: (last - 2 * l + 1, h, 0)))
        args += [steps, steps]
        out_shape += [jax.ShapeDtypeStruct(w_up.shape, w_up.dtype), jax.ShapeDtypeStruct(w_down.shape, w_down.dtype)]
        out_specs += [up_spec, down_spec]
        if held is not None:
            update = 3
            in_specs += [pl.BlockSpec(memory_space=pl.ANY)] * 2
            args += list(held)
            aliases = {5: 0, 6: 1}
    if save:
        out_shape += [jax.ShapeDtypeStruct((n_layers, n_rows, hidden), jnp.bfloat16), jax.ShapeDtypeStruct((n_layers, n_rows, width), jnp.bfloat16)]
        out_specs += [pl.BlockSpec((None, n_rows, tile), lambda l, h: (l, 0, h)), pl.BlockSpec((None, n_rows, width), lambda l, h: (l, 0, 0))]
    out_shape.append(jax.ShapeDtypeStruct((n_rows, width), jnp.bfloat16))
    out_specs.append(whole)
    flops = 4 * n_layers * n_rows * width * hidden
    return pl.pallas_call(
        functools.partial(forward_kernel, save, update, row_chunk(n_rows)),
        out_shape=out_shape,
        grid=(n_layers, hidden // tile),
        in_specs=in_specs,
        out_specs=out_specs,
        scratch_shapes=[
            pltpu.VMEM((n_rows, width), jnp.bfloat16),
            pltpu.VMEM((n_rows, width), jnp.bfloat16),
            pltpu.VMEM((n_rows, width), jnp.float32),
        ],
        input_output_aliases=aliases,
        compiler_params=pltpu.CompilerParams(dimension_semantics=("arbitrary", "arbitrary"), vmem_limit_bytes=VMEM_BYTES),
        cost_estimate=pl.CostEstimate(flops=flops, transcendentals=n_layers * n_rows * hidden, bytes_accessed=n_layers * width * hidden * 16),
        name="forward_next" if update else "forward_now",
    )(*args)


def backward_kernel(need_input, rows_step, n_part, core_ref, x_ref, grad_ref, act_ref, up_ref, down_ref, *refs):
    if need_input:
        out_ref, keep_up, send_up, keep_down, send_down, normed_ref, total_ref, gelu_ref, dpre_ref, tile_ref = refs
    else:
        keep_up, send_up, keep_down, send_down, normed_ref, total_ref, gelu_ref, dpre_ref, tile_ref = refs
    step = pl.program_id(0)
    n_rows = x_ref.shape[0]
    core = core_ref[0]

    @pl.when(step == 0)
    def _():
        for start in range(0, n_rows, rows_step):
            here = slice(start, start + rows_step)
            normed_ref[here, :] = norm_rows(x_ref[here, :].astype(jnp.float32)).astype(jnp.bfloat16)
        if need_input:
            total_ref[...] = jnp.zeros_like(total_ref)

    down_w = down_ref[...].astype(jnp.bfloat16)
    if need_input:
        up_w = up_ref[...].astype(jnp.bfloat16)
    for start in range(0, n_rows, rows_step):
        here = slice(start, start + rows_step)
        dgelu = lax.dot_general(grad_ref[here, :], down_w, CONTRACT_LAST, preferred_element_type=jnp.float32).astype(jnp.bfloat16)
        pre = act_ref[here, :].astype(jnp.float32)
        gelu_v, cdf, tanh_v, squared = gelu_parts(pre)
        gelu_ref[here, :] = gelu_v.astype(jnp.bfloat16)
        slope = cdf + pre * (0.5 - 0.5 * tanh_v * tanh_v) * (TANH_A + (3.0 * TANH_B) * squared)
        dpre = (slope * dgelu.astype(jnp.float32)).astype(jnp.bfloat16)
        dpre_ref[here, :] = dpre
        if need_input:
            total_ref[here, :] += lax.dot_general(dpre, up_w, CONTRACT_LAST, preferred_element_type=jnp.float32)

    n_pairs = tile_ref.shape[0] // (2 * n_part)
    for left, right, keep, send in ((gelu_ref, grad_ref, keep_down, send_down), (dpre_ref, normed_ref, keep_up, send_up)):
        tile_ref[...] = lax.dot_general(left[...], right[...], CONTRACT_ROWS, preferred_element_type=jnp.float32).astype(jnp.bfloat16)
        for pair in range(n_pairs):
            mine = pl.multiple_of((2 * pair + core) * n_part, n_part)
            other = pl.multiple_of((2 * pair + 1 - core) * n_part, n_part)
            keep[pair] = tile_ref[pl.ds(mine, n_part), :]
            send[pair] = tile_ref[pl.ds(other, n_part), :]

    if need_input:
        @pl.when(step == pl.num_programs(0) - 1)
        def _():
            for start in range(0, n_rows, rows_step):
                here = slice(start, start + rows_step)
                cot = total_ref[here, :].astype(jnp.bfloat16).astype(jnp.float32)
                back = norm_rows_back(x_ref[here, :].astype(jnp.float32), cot)
                out_ref[here, :] = (grad_ref[here, :].astype(jnp.float32) + back).astype(jnp.bfloat16)


def backward_block(layer, core, saved_x, saved_act, w_up, w_down, grad_rows, n_part, need_input):
    n_rows, width = grad_rows.shape
    hidden = w_up.shape[2]
    tile = tile_of(hidden)
    whole = pl.BlockSpec((n_rows, width), lambda h, c: (0, 0), pipeline_mode=pl.Buffered(1))
    n_pairs = tile // (2 * n_part)
    half = jax.ShapeDtypeStruct((hidden // (2 * n_part), n_part, width), jnp.bfloat16)
    half_spec = pl.BlockSpec((n_pairs, n_part, width), lambda h, c: (h, 0, 0))
    out_shape = [half] * 4
    out_specs = [half_spec] * 4
    if need_input:
        out_shape = [jax.ShapeDtypeStruct((n_rows, width), jnp.bfloat16)] + out_shape
        out_specs = [pl.BlockSpec((n_rows, width), lambda h, c: (0, 0))] + out_specs
    flops = (8 if need_input else 6) * n_rows * width * hidden
    outs = pl.pallas_call(
        functools.partial(backward_kernel, need_input, row_chunk(n_rows), n_part),
        out_shape=out_shape,
        grid_spec=pltpu.PrefetchScalarGridSpec(
            num_scalar_prefetch=1,
            grid=(hidden // tile,),
            in_specs=[
                pl.BlockSpec((None, n_rows, width), lambda h, c: (layer, 0, 0), pipeline_mode=pl.Buffered(1)),
                whole,
                pl.BlockSpec((None, n_rows, tile), lambda h, c: (layer, 0, h)),
                pl.BlockSpec((None, width, tile), lambda h, c: (layer, 0, h)),
                pl.BlockSpec((None, tile, width), lambda h, c: (layer, h, 0)),
            ],
            out_specs=out_specs,
            scratch_shapes=[
                pltpu.VMEM((n_rows, width), jnp.bfloat16),
                pltpu.VMEM((n_rows, width), jnp.float32),
                pltpu.VMEM((n_rows, tile), jnp.bfloat16),
                pltpu.VMEM((n_rows, tile), jnp.bfloat16),
                pltpu.VMEM((tile, width), jnp.bfloat16),
            ],
        ),
        compiler_params=pltpu.CompilerParams(dimension_semantics=("arbitrary",), vmem_limit_bytes=VMEM_BYTES),
        cost_estimate=pl.CostEstimate(flops=flops, transcendentals=n_rows * hidden, bytes_accessed=width * hidden * 16),
        name="backward_block",
    )(core, saved_x, grad_rows, saved_act, w_up, w_down)
    if need_input:
        return outs
    return [None] + list(outs)


def add_bf16(left, right):
    return (left.astype(jnp.float32) + right.astype(jnp.float32)).astype(jnp.bfloat16)


def exchange(values, bit, n_dev):
    return lax.ppermute(values, "data", [(d, d ^ (1 << bit)) for d in range(n_dev)])


class HalvingSum:
    def __init__(self, keep, send, order, index, n_dev):
        self.order, self.index, self.n_dev = order, index, n_dev
        self.left = sorted(order, reverse=True)
        self.kept, self.sent, self.bit = keep, send, 0
        self.stage = 0
        self.total = None

    def launch(self):
        self.received = exchange(self.sent, self.bit, self.n_dev)

    def land(self):
        total = add_bf16(self.kept, self.received)
        if self.stage == 0:
            total = total.reshape((2,) * len(self.left) + total.shape[1:])
        if self.stage == len(self.order):
            self.total = total
            return
        self.bit = self.order[self.stage]
        spot = self.left.index(self.bit)
        mine = (self.index >> self.bit) & 1
        self.sent = lax.dynamic_index_in_dim(total, 1 - mine, spot, keepdims=False)
        self.kept = lax.dynamic_index_in_dim(total, mine, spot, keepdims=False)
        self.left.remove(self.bit)
        self.stage += 1


def layer_groups(n_layers):
    singles = max(n_layers - 4, 0)
    groups = [[n_layers - 1 - k] for k in range(singles)]
    rest = list(range(n_layers - 1 - singles, 0, -1))
    if rest:
        groups.append(rest)
    return groups + [[0]]


def tie(first, others):
    tied = lax.optimization_barrier((first, tuple(others)))
    return tied[0], list(tied[1])


def head_forward(rows, head_b, n_img):
    pooled = jnp.mean(rows.reshape(n_img, -1, rows.shape[-1]), axis=1, dtype=jnp.float32)
    normed = norm_rows(pooled).astype(jnp.bfloat16)
    return jnp.dot(normed, head_b, preferred_element_type=jnp.float32), pooled, normed


def solution(mesh):
    n_dev = mesh.shape["data"]

    def local_step(x_now, x_next, labels, w_up, w_down, w_head, mom_up, mom_down, mom_head, learn_rate, mom_decay):
        n_img, n_tok, width = x_now.shape
        n_layers = w_up.shape[0]
        batch_total = n_img * n_dev
        shard_index = lax.axis_index("data")
        core = (shard_index % 2).astype(jnp.int32).reshape(1)
        head_b = w_head.astype(jnp.bfloat16)
        saved_act, saved_x, rows = forward_stack(x_now.reshape(n_img * n_tok, width), w_up, w_down, list(range(n_layers)), True)
        logits, pooled, normed = head_forward(rows, head_b, n_img)
        soft_probs = jax.nn.softmax(logits, axis=-1)
        targets = jax.nn.one_hot(labels, logits.shape[-1], dtype=jnp.float32)
        grad_logits = ((soft_probs - targets) / batch_total).astype(jnp.bfloat16)
        head_grad = lax.dot_general(normed, grad_logits, CONTRACT_ROWS, preferred_element_type=jnp.float32).astype(jnp.bfloat16)
        grad_normed = lax.dot_general(grad_logits, head_b, CONTRACT_LAST, preferred_element_type=jnp.float32).astype(jnp.bfloat16)
        _, norm_pull = jax.vjp(norm_rows, pooled)
        grad_pooled = norm_pull(grad_normed.astype(jnp.float32))[0]
        grad_rows = jnp.broadcast_to((grad_pooled / n_tok)[:, None, :], (n_img, n_tok, width))
        grad_rows = grad_rows.astype(jnp.bfloat16).reshape(n_img * n_tok, width)

        head_sum = lax.psum_scatter(head_grad, "data", scatter_dimension=0, tiled=True)
        head_width = mom_head.shape[0]
        n_part = mom_down.shape[1]
        turns = [(1, 2, 3), (2, 3, 1), (3, 1, 2)]
        moms_up = [None] * n_layers
        moms_down = [None] * n_layers
        steps_of = {}
        groups = layer_groups(n_layers)
        flying = []
        gathering = []

        def collect(first, age):
            ready = [entry for entry in gathering if entry[1] >= age]
            if ready:
                first, landed = tie(first, [steps_of[key] for key, _ in ready])
                for (key, _), value in zip(ready, landed):
                    steps_of[key] = value
            for entry in ready:
                gathering.remove(entry)
            for entry in gathering:
                entry[1] += 1
            return first

        def advance(flying, grad_rows):
            grad_rows, landed = tie(grad_rows, [part.received for _, pair in flying for part in pair])
            still, done = [], []
            for layer, pair in flying:
                for part in pair:
                    part.received = landed.pop(0)
                    part.land()
                (done if pair[0].total is not None else still).append((layer, pair))
            for layer, pair in done:
                up_sum, down_sum = pair[0].total, pair[1].total
                moms_up[layer] = mom_decay * mom_up[layer].T + up_sum.astype(jnp.float32)
                moms_down[layer] = mom_decay * mom_down[layer] + down_sum.astype(jnp.float32)
            for group in groups:
                if tuple(group) not in steps_of and all(moms_up[layer] is not None for layer in group):
                    sent = []
                    for layer in group:
                        sent.append((learn_rate * moms_up[layer]).astype(jnp.bfloat16))
                        sent.append((learn_rate * moms_down[layer]).astype(jnp.bfloat16))
                    grad_rows, packed = tie(grad_rows, [jnp.stack(sent)])
                    if group[-1] == 0:
                        packed[0] = collect(packed[0], 1)
                    gathering.append([tuple(group), 0])
                    steps_of[tuple(group)] = lax.all_gather(packed[0], "data", axis=1, tiled=True)
            return still, grad_rows

        def launch(flying, grad_rows):
            grad_rows, sent = tie(grad_rows, [part.sent for _, pair in flying for part in pair])
            for _, pair in flying:
                for part in pair:
                    part.sent = sent.pop(0)
                    part.launch()
            return grad_rows

        for layer in range(n_layers - 1, -1, -1):
            grad_next, keep_up, send_up, keep_down, send_down = backward_block(
                layer, core, saved_x, saved_act, w_up, w_down, grad_rows, n_part, layer > 0)
            grad_rows = keep_up if grad_next is None else grad_next
            if layer == n_layers - 1:
                grad_rows, waited = tie(grad_rows, [head_sum])
                new_mom_head = mom_decay * mom_head + waited[0].astype(jnp.float32)
                head_part = lax.dynamic_slice_in_dim(w_head, shard_index * head_width, head_width, axis=0) - learn_rate * new_mom_head
                grad_rows, waited = tie(grad_rows, [head_part])
                new_w_head = lax.all_gather(waited[0], "data", axis=0, tiled=True)
            if layer == n_layers - 2:
                grad_rows, waited = tie(grad_rows, [new_w_head])
                new_w_head = waited[0]
            grad_rows = collect(grad_rows, 2)
            flying, grad_rows = advance(flying, grad_rows)
            if grad_next is None:
                keep_up = grad_rows
            flying.append((layer, (
                HalvingSum(keep_up, send_up, turns[layer % 3], shard_index, n_dev),
                HalvingSum(keep_down, send_down, turns[(layer + 1) % 3], shard_index, n_dev))))
            grad_rows = launch(flying, grad_rows)
        token = mom_decay
        while flying:
            flying, token = advance(flying, token)
            if flying:
                token = launch(flying, token)

        next_rows = x_next.reshape(n_img * n_tok, width)
        held = None
        for group in reversed(groups):
            steps = steps_of[tuple(group)]
            new_up, new_down, next_rows = forward_stack(next_rows, w_up, w_down, group[::-1], False, steps, held)
            held = (new_up, new_down)
        logits_next = head_forward(next_rows, new_w_head.astype(jnp.bfloat16), n_img)[0]
        new_mom_up = jnp.stack(moms_up).transpose(0, 2, 1)
        return (logits_next, held[0], held[1], new_w_head, new_mom_up, jnp.stack(moms_down), new_mom_head)

    spec_up = P(None, None, "data")
    spec_down = P(None, "data", None)
    spec_head = P("data", None)
    return jax.shard_map(
        local_step,
        mesh=mesh,
        in_specs=(P("data"), P("data"), P("data"), P(), P(), P(), spec_up, spec_down, spec_head, P(), P()),
        out_specs=(P("data"), P(), P(), P(), spec_up, spec_down, spec_head),
        check_vma=False,
    )
```

```python
import functools

import jax
import jax.numpy as jnp
from jax import lax
from jax.experimental import pallas as pl
from jax.experimental.pallas import tpu as pltpu
from jax.sharding import PartitionSpec as P

LN_EPS = 1e-6
CONTRACT_ROWS = (((0,), (0,)), ((), ()))
CONTRACT_LAST = (((1,), (1,)), ((), ()))
TANH_A = 0.7978845608028654
TANH_B = 0.7978845608028654 * 0.044715
VMEM_BYTES = 67000000


def norm_rows(values):
    mean_v = jnp.mean(values, axis=-1, keepdims=True)
    centered = values - mean_v
    var_v = jnp.mean(centered * centered, axis=-1, keepdims=True)
    return centered * lax.rsqrt(var_v + LN_EPS)


def norm_rows_back(values, cot):
    mean_v = jnp.mean(values, axis=-1, keepdims=True)
    centered = values - mean_v
    var_v = jnp.mean(centered * centered, axis=-1, keepdims=True)
    rstd = lax.rsqrt(var_v + LN_EPS)
    hat = centered * rstd
    mean_c = jnp.mean(cot, axis=-1, keepdims=True)
    mean_h = jnp.mean(cot * hat, axis=-1, keepdims=True)
    return rstd * (cot - mean_c - hat * mean_h)


def gelu_parts(values):
    squared = values * values
    tanh_v = jnp.tanh(values * (TANH_A + TANH_B * squared))
    cdf = 0.5 + 0.5 * tanh_v
    return values * cdf, cdf, tanh_v, squared


def row_chunk(n_rows):
    for size in (224, 256, 128, 64, 32, 16):
        if n_rows % size == 0:
            return size
    return n_rows


def tile_of(hidden):
    for size in (768, 384):
        if hidden % size == 0:
            return size
    return hidden


def forward_kernel(save, update, rows_step, *refs):
    refs = list(refs)
    x_ref, up_ref, down_ref = refs[:3]
    refs = refs[3:]
    if update:
        step_up_ref, step_down_ref = refs[:2]
        refs = refs[2:]
        refs = refs[update - 1:]
        new_up_ref, new_down_ref = refs[:2]
        refs = refs[2:]
    if save:
        act_ref, saved_ref = refs[:2]
        refs = refs[2:]
    out_ref, rows_ref, normed_ref, total_ref = refs
    layer, tile = pl.program_id(0), pl.program_id(1)
    n_rows = x_ref.shape[0]

    @pl.when((layer == 0) & (tile == 0))
    def _():
        rows_ref[...] = x_ref[...]

    @pl.when(tile == 0)
    def _():
        for start in range(0, n_rows, rows_step):
            part = rows_ref[start:start + rows_step, :]
            normed_ref[start:start + rows_step, :] = norm_rows(part.astype(jnp.float32)).astype(jnp.bfloat16)
            if save:
                saved_ref[start:start + rows_step, :] = part
        total_ref[...] = jnp.zeros_like(total_ref)

    up_w = up_ref[...]
    down_w = down_ref[...]
    if update:
        up_w = up_w - step_up_ref[...].astype(jnp.float32).T
        down_w = down_w - step_down_ref[...].astype(jnp.float32)
        new_up_ref[...] = up_w
        new_down_ref[...] = down_w
    up_w = up_w.astype(jnp.bfloat16)
    down_w = down_w.astype(jnp.bfloat16)
    for start in range(0, n_rows, rows_step):
        here = slice(start, start + rows_step)
        pre = jnp.dot(normed_ref[here, :], up_w, preferred_element_type=jnp.float32).astype(jnp.bfloat16)
        if save:
            act_ref[here, :] = pre
        gelu_v = gelu_parts(pre.astype(jnp.float32))[0].astype(jnp.bfloat16)
        total_ref[here, :] += jnp.dot(gelu_v, down_w, preferred_element_type=jnp.float32)

    @pl.when(tile == pl.num_programs(1) - 1)
    def _():
        for start in range(0, n_rows, rows_step):
            here = slice(start, start + rows_step)
            block = total_ref[here, :].astype(jnp.bfloat16).astype(jnp.float32)
            rows_ref[here, :] = (rows_ref[here, :].astype(jnp.float32) + block).astype(jnp.bfloat16)

    @pl.when((tile == pl.num_programs(1) - 1) & (layer == pl.num_programs(0) - 1))
    def _():
        out_ref[...] = rows_ref[...]


def forward_stack(x_rows, w_up, w_down, layers, save, steps=None, held=None):
    n_rows, width = x_rows.shape
    hidden = w_up.shape[2]
    tile = tile_of(hidden)
    first, n_layers = layers[0], len(layers)
    whole = pl.BlockSpec((n_rows, width), lambda l, h: (0, 0))
    up_spec = pl.BlockSpec((None, width, tile), lambda l, h: (first + l, 0, h))
    down_spec = pl.BlockSpec((None, tile, width), lambda l, h: (first + l, h, 0))
    in_specs = [whole, up_spec, down_spec]
    args = [x_rows, w_up, w_down]
    out_shape, out_specs, aliases = [], [], {}
    update = 0
    if steps is not None:
        update = 1
        last = 2 * (n_layers - 1)
        in_specs.append(pl.BlockSpec((None, tile, width), lambda l, h: (last - 2 * l, h, 0)))
        in_specs.append(pl.BlockSpec((None, tile, width), lambda l, h: (last - 2 * l + 1, h, 0)))
        args += [steps, steps]
        out_shape += [jax.ShapeDtypeStruct(w_up.shape, w_up.dtype), jax.ShapeDtypeStruct(w_down.shape, w_down.dtype)]
        out_specs += [up_spec, down_spec]
        if held is not None:
            update = 3
            in_specs += [pl.BlockSpec(memory_space=pl.ANY)] * 2
            args += list(held)
            aliases = {5: 0, 6: 1}
    if save:
        out_shape += [jax.ShapeDtypeStruct((n_layers, n_rows, hidden), jnp.bfloat16), jax.ShapeDtypeStruct((n_layers, n_rows, width), jnp.bfloat16)]
        out_specs += [pl.BlockSpec((None, n_rows, tile), lambda l, h: (l, 0, h)), pl.BlockSpec((None, n_rows, width), lambda l, h: (l, 0, 0))]
    out_shape.append(jax.ShapeDtypeStruct((n_rows, width), jnp.bfloat16))
    out_specs.append(whole)
    flops = 4 * n_layers * n_rows * width * hidden
    return pl.pallas_call(
        functools.partial(forward_kernel, save, update, row_chunk(n_rows)),
        out_shape=out_shape,
        grid=(n_layers, hidden // tile),
        in_specs=in_specs,
        out_specs=out_specs,
        scratch_shapes=[
            pltpu.VMEM((n_rows, width), jnp.bfloat16),
            pltpu.VMEM((n_rows, width), jnp.bfloat16),
            pltpu.VMEM((n_rows, width), jnp.float32),
        ],
        input_output_aliases=aliases,
        compiler_params=pltpu.CompilerParams(dimension_semantics=("arbitrary", "arbitrary"), vmem_limit_bytes=VMEM_BYTES),
        cost_estimate=pl.CostEstimate(flops=flops, transcendentals=n_layers * n_rows * hidden, bytes_accessed=n_layers * width * hidden * 16),
        name="forward_next" if update else "forward_now",
    )(*args)


def backward_kernel(need_input, rows_step, n_part, core_ref, x_ref, grad_ref, act_ref, up_ref, down_ref, *refs):
    if need_input:
        out_ref, keep_up, send_up, keep_down, send_down, normed_ref, total_ref, gelu_ref, dpre_ref, tile_ref = refs
    else:
        keep_up, send_up, keep_down, send_down, normed_ref, total_ref, gelu_ref, dpre_ref, tile_ref = refs
    step = pl.program_id(0)
    n_rows = x_ref.shape[0]
    core = core_ref[0]

    @pl.when(step == 0)
    def _():
        for start in range(0, n_rows, rows_step):
            here = slice(start, start + rows_step)
            normed_ref[here, :] = norm_rows(x_ref[here, :].astype(jnp.float32)).astype(jnp.bfloat16)
        if need_input:
            total_ref[...] = jnp.zeros_like(total_ref)

    down_w = down_ref[...].astype(jnp.bfloat16)
    if need_input:
        up_w = up_ref[...].astype(jnp.bfloat16)
    for start in range(0, n_rows, rows_step):
        here = slice(start, start + rows_step)
        dgelu = lax.dot_general(grad_ref[here, :], down_w, CONTRACT_LAST, preferred_element_type=jnp.float32).astype(jnp.bfloat16)
        pre = act_ref[here, :].astype(jnp.float32)
        gelu_v, cdf, tanh_v, squared = gelu_parts(pre)
        gelu_ref[here, :] = gelu_v.astype(jnp.bfloat16)
        slope = cdf + pre * (0.5 - 0.5 * tanh_v * tanh_v) * (TANH_A + (3.0 * TANH_B) * squared)
        dpre = (slope * dgelu.astype(jnp.float32)).astype(jnp.bfloat16)
        dpre_ref[here, :] = dpre
        if need_input:
            total_ref[here, :] += lax.dot_general(dpre, up_w, CONTRACT_LAST, preferred_element_type=jnp.float32)

    n_pairs = tile_ref.shape[0] // (2 * n_part)
    for left, right, keep, send in ((gelu_ref, grad_ref, keep_down, send_down), (dpre_ref, normed_ref, keep_up, send_up)):
        tile_ref[...] = lax.dot_general(left[...], right[...], CONTRACT_ROWS, preferred_element_type=jnp.float32).astype(jnp.bfloat16)
        for pair in range(n_pairs):
            mine = pl.multiple_of((2 * pair + core) * n_part, n_part)
            other = pl.multiple_of((2 * pair + 1 - core) * n_part, n_part)
            keep[pair] = tile_ref[pl.ds(mine, n_part), :]
            send[pair] = tile_ref[pl.ds(other, n_part), :]

    if need_input:
        @pl.when(step == pl.num_programs(0) - 1)
        def _():
            for start in range(0, n_rows, rows_step):
                here = slice(start, start + rows_step)
                cot = total_ref[here, :].astype(jnp.bfloat16).astype(jnp.float32)
                back = norm_rows_back(x_ref[here, :].astype(jnp.float32), cot)
                out_ref[here, :] = (grad_ref[here, :].astype(jnp.float32) + back).astype(jnp.bfloat16)


def backward_block(layer, core, saved_x, saved_act, w_up, w_down, grad_rows, n_part, need_input):
    n_rows, width = grad_rows.shape
    hidden = w_up.shape[2]
    tile = tile_of(hidden)
    whole = pl.BlockSpec((n_rows, width), lambda h, c: (0, 0), pipeline_mode=pl.Buffered(1))
    n_pairs = tile // (2 * n_part)
    half = jax.ShapeDtypeStruct((hidden // (2 * n_part), n_part, width), jnp.bfloat16)
    half_spec = pl.BlockSpec((n_pairs, n_part, width), lambda h, c: (h, 0, 0))
    out_shape = [half] * 4
    out_specs = [half_spec] * 4
    if need_input:
        out_shape = [jax.ShapeDtypeStruct((n_rows, width), jnp.bfloat16)] + out_shape
        out_specs = [pl.BlockSpec((n_rows, width), lambda h, c: (0, 0))] + out_specs
    flops = (8 if need_input else 6) * n_rows * width * hidden
    outs = pl.pallas_call(
        functools.partial(backward_kernel, need_input, row_chunk(n_rows), n_part),
        out_shape=out_shape,
        grid_spec=pltpu.PrefetchScalarGridSpec(
            num_scalar_prefetch=1,
            grid=(hidden // tile,),
            in_specs=[
                pl.BlockSpec((None, n_rows, width), lambda h, c: (layer, 0, 0), pipeline_mode=pl.Buffered(1)),
                whole,
                pl.BlockSpec((None, n_rows, tile), lambda h, c: (layer, 0, h)),
                pl.BlockSpec((None, width, tile), lambda h, c: (layer, 0, h)),
                pl.BlockSpec((None, tile, width), lambda h, c: (layer, h, 0)),
            ],
            out_specs=out_specs,
            scratch_shapes=[
                pltpu.VMEM((n_rows, width), jnp.bfloat16),
                pltpu.VMEM((n_rows, width), jnp.float32),
                pltpu.VMEM((n_rows, tile), jnp.bfloat16),
                pltpu.VMEM((n_rows, tile), jnp.bfloat16),
                pltpu.VMEM((tile, width), jnp.bfloat16),
            ],
        ),
        compiler_params=pltpu.CompilerParams(dimension_semantics=("arbitrary",), vmem_limit_bytes=VMEM_BYTES),
        cost_estimate=pl.CostEstimate(flops=flops, transcendentals=n_rows * hidden, bytes_accessed=width * hidden * 16),
        name="backward_block",
    )(core, saved_x, grad_rows, saved_act, w_up, w_down)
    if need_input:
        return outs
    return [None] + list(outs)


def add_bf16(left, right):
    return (left.astype(jnp.float32) + right.astype(jnp.float32)).astype(jnp.bfloat16)


def exchange(values, bit, n_dev):
    return lax.ppermute(values, "data", [(d, d ^ (1 << bit)) for d in range(n_dev)])


class HalvingSum:
    def __init__(self, keep, send, order, index, n_dev):
        self.order, self.index, self.n_dev = order, index, n_dev
        self.left = sorted(order, reverse=True)
        self.kept, self.sent, self.bit = keep, send, 0
        self.stage = 0
        self.total = None

    def launch(self):
        self.received = exchange(self.sent, self.bit, self.n_dev)

    def land(self):
        kept, received = self.kept, self.received
        if self.stage == len(self.order):
            self.total = add_bf16(kept, received)
            return
        if self.stage == 0:
            kept = kept.reshape((2,) * len(self.left) + kept.shape[1:])
            received = received.reshape(kept.shape)
        self.bit = self.order[self.stage]
        spot = self.left.index(self.bit)
        mine = (self.index >> self.bit) & 1
        self.sent = add_bf16(*(lax.dynamic_index_in_dim(v, 1 - mine, spot, keepdims=False) for v in (kept, received)))
        self.kept = add_bf16(*(lax.dynamic_index_in_dim(v, mine, spot, keepdims=False) for v in (kept, received)))
        self.left.remove(self.bit)
        self.stage += 1


def layer_groups(n_layers):
    return [[layer] for layer in range(n_layers - 1, -1, -1)]


def tie(first, others):
    tied = lax.optimization_barrier((first, tuple(others)))
    return tied[0], list(tied[1])


def head_forward(rows, head_b, n_img):
    pooled = jnp.mean(rows.reshape(n_img, -1, rows.shape[-1]), axis=1, dtype=jnp.float32)
    normed = norm_rows(pooled).astype(jnp.bfloat16)
    return jnp.dot(normed, head_b, preferred_element_type=jnp.float32), pooled, normed


def solution(mesh):
    n_dev = mesh.shape["data"]

    def local_step(x_now, x_next, labels, w_up, w_down, w_head, mom_up, mom_down, mom_head, learn_rate, mom_decay):
        n_img, n_tok, width = x_now.shape
        n_layers = w_up.shape[0]
        batch_total = n_img * n_dev
        shard_index = lax.axis_index("data")
        core = (shard_index % 2).astype(jnp.int32).reshape(1)
        head_b = w_head.astype(jnp.bfloat16)
        saved_act, saved_x, rows = forward_stack(x_now.reshape(n_img * n_tok, width), w_up, w_down, list(range(n_layers)), True)
        logits, pooled, normed = head_forward(rows, head_b, n_img)
        soft_probs = jax.nn.softmax(logits, axis=-1)
        targets = jax.nn.one_hot(labels, logits.shape[-1], dtype=jnp.float32)
        grad_logits = ((soft_probs - targets) / batch_total).astype(jnp.bfloat16)
        head_grad = lax.dot_general(normed, grad_logits, CONTRACT_ROWS, preferred_element_type=jnp.float32).astype(jnp.bfloat16)
        grad_normed = lax.dot_general(grad_logits, head_b, CONTRACT_LAST, preferred_element_type=jnp.float32).astype(jnp.bfloat16)
        _, norm_pull = jax.vjp(norm_rows, pooled)
        grad_pooled = norm_pull(grad_normed.astype(jnp.float32))[0]
        grad_rows = jnp.broadcast_to((grad_pooled / n_tok)[:, None, :], (n_img, n_tok, width))
        grad_rows = grad_rows.astype(jnp.bfloat16).reshape(n_img * n_tok, width)

        head_sum = lax.psum_scatter(head_grad, "data", scatter_dimension=0, tiled=True)
        head_width = mom_head.shape[0]
        n_part = mom_down.shape[1]
        turns = [(1, 2, 3), (2, 3, 1), (3, 1, 2)]
        moms_up = [None] * n_layers
        moms_down = [None] * n_layers
        steps_of = {}
        groups = layer_groups(n_layers)
        flying = []
        gathering = []

        def collect(first, age, lowest=0):
            ready = [entry for entry in gathering if entry[1] >= age and entry[0][-1] >= lowest]
            if ready:
                first, landed = tie(first, [steps_of[key] for key, _ in ready])
                for (key, _), value in zip(ready, landed):
                    steps_of[key] = value
            for entry in ready:
                gathering.remove(entry)
            for entry in gathering:
                entry[1] += 1
            return first

        def advance(flying, grad_rows):
            grad_rows, landed = tie(grad_rows, [part.received for _, pair in flying for part in pair])
            still, done = [], []
            for layer, pair in flying:
                for part in pair:
                    part.received = landed.pop(0)
                    part.land()
                (done if pair[0].total is not None else still).append((layer, pair))
            for layer, pair in done:
                up_sum, down_sum = pair[0].total, pair[1].total
                moms_up[layer] = mom_decay * mom_up[layer].T + up_sum.astype(jnp.float32)
                moms_down[layer] = mom_decay * mom_down[layer] + down_sum.astype(jnp.float32)
            for group in groups:
                if tuple(group) not in steps_of and all(moms_up[layer] is not None for layer in group):
                    sent = []
                    for layer in group:
                        sent.append((learn_rate * moms_up[layer]).astype(jnp.bfloat16))
                        sent.append((learn_rate * moms_down[layer]).astype(jnp.bfloat16))
                    grad_rows, packed = tie(grad_rows, [jnp.stack(sent)])
                    if group[-1] == 0:
                        packed[0] = collect(packed[0], 0, 3)
                    gathering.append([tuple(group), 0])
                    steps_of[tuple(group)] = lax.all_gather(packed[0], "data", axis=1, tiled=True)
            return still, grad_rows

        def launch(flying, grad_rows):
            grad_rows, sent = tie(grad_rows, [part.sent for _, pair in flying for part in pair])
            for _, pair in flying:
                for part in pair:
                    part.sent = sent.pop(0)
                    part.launch()
            return grad_rows

        for layer in range(n_layers - 1, -1, -1):
            grad_next, keep_up, send_up, keep_down, send_down = backward_block(
                layer, core, saved_x, saved_act, w_up, w_down, grad_rows, n_part, layer > 0)
            grad_rows = keep_up if grad_next is None else grad_next
            if layer == n_layers - 1:
                grad_rows, waited = tie(grad_rows, [head_sum])
                new_mom_head = mom_decay * mom_head + waited[0].astype(jnp.float32)
                head_part = lax.dynamic_slice_in_dim(w_head, shard_index * head_width, head_width, axis=0) - learn_rate * new_mom_head
                grad_rows, waited = tie(grad_rows, [head_part])
                new_w_head = lax.all_gather(waited[0], "data", axis=0, tiled=True)
            if layer == n_layers - 2:
                grad_rows, waited = tie(grad_rows, [new_w_head])
                new_w_head = waited[0]
            grad_rows = collect(grad_rows, 2)
            flying, grad_rows = advance(flying, grad_rows)
            if grad_next is None:
                keep_up = grad_rows
            flying.append((layer, (
                HalvingSum(keep_up, send_up, turns[layer % 3], shard_index, n_dev),
                HalvingSum(keep_down, send_down, turns[(layer + 1) % 3], shard_index, n_dev))))
            grad_rows = launch(flying, grad_rows)
        token = mom_decay
        while flying:
            if len(flying) == 1:
                last = flying[0][1][0]
                last.received = collect(last.received, 0, 3)
            flying, token = advance(flying, token)
            if flying:
                token = launch(flying, token)

        next_rows = x_next.reshape(n_img * n_tok, width)
        held = None
        for group in reversed(groups):
            steps = steps_of[tuple(group)]
            new_up, new_down, next_rows = forward_stack(next_rows, w_up, w_down, group[::-1], False, steps, held)
            held = (new_up, new_down)
        logits_next = head_forward(next_rows, new_w_head.astype(jnp.bfloat16), n_img)[0]
        new_mom_up = jnp.stack(moms_up).transpose(0, 2, 1)
        return (logits_next, held[0], held[1], new_w_head, new_mom_up, jnp.stack(moms_down), new_mom_head)

    spec_up = P(None, None, "data")
    spec_down = P(None, "data", None)
    spec_head = P("data", None)
    return jax.shard_map(
        local_step,
        mesh=mesh,
        in_specs=(P("data"), P("data"), P("data"), P(), P(), P(), spec_up, spec_down, spec_head, P(), P()),
        out_specs=(P("data"), P(), P(), P(), spec_up, spec_down, spec_head),
        check_vma=False,
    )
```
